32 devices in a mesh: grp: 4 (over y, x), mem: 8 (over z, core).
Axes of the slice: x: 2, y: 2, z: 4, core: 2. Of those that a mesh axis runs over, the one named last changes fastest.
Arguments:
- params: float32 [4, 2048, 2048], P('grp', 'mem'), may hold values from -6 to 6
- estimate: float32 [4, 2048, 2048], P('grp', 'mem'), may hold values from -6 to 6
- mixed_sum: float32 [4, 2048, 2048], P('grp', 'mem'), may hold values from -6 to 6
- activations: bfloat16 [32768, 2048], P(('grp', 'mem')), may hold values from -6 to 6
- out_grads: bfloat16 [32768, 2048], P(('grp', 'mem')), may hold values from -6 to 6
- exponents: int32 [4, 32], P('grp', 'mem'), may hold values from 0 to 3
- edge_weight: float32 [4], replicated, may hold values from 0.1 to 0.45
Outputs:
- new_params: float32 [4, 2048, 2048], P('grp', 'mem')
- new_estimate: float32 [4, 2048, 2048], P('grp', 'mem')
- new_mixed: float32 [4, 2048, 2048], P('grp', 'mem')
The draws below stay inside these ranges and needn't reach their ends.
All inputs are finite; a program needn't handle non-finite values.
Results may differ from the reference program's by a relative error of at most 0.01.
Values may be sent and summed in bfloat16 or wider, within the bound.
A program may use at most 128 MiB of HBM per device.

```python
import math
import jax
import jax.numpy as jnp
from jax import lax

D = 2048
INNER = 2048
TOK_DEV = 1024
BLOCK = 64
GROUPS = 4
ROWS = 32768
N_MEM = 8


def plant(entries, key, low, top_value):
    spot = [jax.random.randint(jax.random.fold_in(key, axis), (), 0, length) for axis, length in enumerate(entries.shape)]
    longest = entries.shape.index(max(entries.shape))
    neighbour = spot[:longest] + [(spot[longest] + 1) % entries.shape[longest]] + spot[longest + 1:]
    return entries.at[tuple(spot)].set(low).at[tuple(neighbour)].set(top_value)


def strengthened(array, stream_key, source, target, blocks, factor):
    def block_of(dim):
        return (jnp.arange(array.shape[dim]) // (array.shape[dim] // blocks)).reshape((-1,) + (1,) * (array.ndim - 1 - dim))

    first = jax.random.permutation(stream_key, blocks)[block_of(target)]
    second = (block_of(target) + blocks // 2) % blocks
    return jnp.where((block_of(source) == first) | (block_of(source) == second), factor * array, array)


def block_scale(stream_key, shape, cuts, smallest, largest):
    loudness, own = 1.0, jax.random.fold_in(stream_key, 6)
    for dim, shards_of in cuts:
        steps = jnp.exp(jax.random.uniform(jax.random.fold_in(own, dim), (shards_of,), jnp.float32, smallest / len(cuts), largest / len(cuts)))
        loudness = loudness * jnp.repeat(steps, shape[dim] // shards_of).reshape([-1 if axis == dim else 1 for axis in range(len(shape))])
    return loudness


def scatter_about(key, extent, scale, bound, pieces=(), dtype=jnp.bfloat16):
    drawn = jax.random.normal(key, extent, jnp.float32) * scale
    if len(pieces) > 0:
        drawn = block_scale(key, extent, pieces, -0.22, 0.18) * drawn
    return jnp.clip(drawn, min=-bound, max=bound).astype(dtype)


def gaussian_with(own_key, extent, spread, most, pieces, heavy, dtype=jnp.bfloat16):
    entries = spread * jax.random.normal(own_key, extent, jnp.float32)
    if pieces:
        entries = entries * block_scale(own_key, extent, pieces, -0.22, 0.18)
    return jnp.clip(strengthened(entries, jax.random.fold_in(own_key, 3), *heavy), -most, most).astype(dtype)


def setup_inputs(seed: int = 0) -> dict:
    key_list = jax.random.split(jax.random.key(seed), 8)
    params = scatter_about(key_list[0], (GROUPS, D, INNER), 1.0, 6.0, ((0, 4), (1, 8)), jnp.float32)
    estimate = scatter_about(key_list[1], (GROUPS, D, INNER), 1.0, 6.0, ((0, 4), (1, 8)), jnp.float32)
    mixed_sum = scatter_about(key_list[2], (GROUPS, D, INNER), 1.0, 6.0, ((0, 4), (1, 8)), jnp.float32)
    activations = gaussian_with(key_list[3], (ROWS, D), 1.0, 6.0, ((0, 32),), (0, 1, 32, 2.75))
    out_grads = scatter_about(key_list[4], (ROWS, INNER), 1.0, 6.0, ((0, 32),))
    exponents = plant(jax.random.randint(key_list[5], (GROUPS, D // BLOCK), 0, 4), jax.random.fold_in(key_list[5], 1), 0, 3).astype(jnp.int32)
    edge_weight = jnp.clip(jax.random.uniform(key_list[6], (GROUPS,), jnp.float32, 0.1, 0.45), 0.1, 0.45)
    return dict(params=params, estimate=estimate, mixed_sum=mixed_sum, activations=activations, out_grads=out_grads, exponents=exponents, edge_weight=edge_weight)


step_size = 0.5
mixing_rate = 0.4

def reference(params, estimate, mixed_sum, activations, out_grads, exponents, edge_weight):
    groups = params.shape[0]
    group_acts = activations.reshape(groups, N_MEM, TOK_DEV, D)
    group_outs = out_grads.reshape(groups, N_MEM, TOK_DEV, INNER)

    def group_gradient(blocks):

        def accumulate(running, member):
            partial_value = lax.dot_general(member[0], member[1], (((0,), (0,)), ((), ())), preferred_element_type=jnp.float32)
            rounded = lax.optimization_barrier(partial_value.astype(jnp.bfloat16))
            return (running + rounded.astype(jnp.float32), None)
        running, _ = lax.scan(accumulate, jnp.zeros((D, INNER), jnp.float32), blocks)
        return running
    gradient = lax.map(group_gradient, (group_acts, group_outs))
    factor = step_size / math.sqrt(N_MEM * TOK_DEV)
    stepped = params - factor * gradient
    change = stepped - estimate
    scales = jnp.exp2(exponents.astype(jnp.float32))[:, :, None, None]
    blocked = change.reshape(groups, D // BLOCK, BLOCK, INNER)
    levels = lax.optimization_barrier(jnp.clip(blocked / scales, -1.0, 1.0).astype(jnp.bfloat16))
    compressed = (levels.astype(jnp.float32) * scales).astype(jnp.bfloat16).reshape(groups, D, INNER)
    own_piece = compressed.astype(jnp.float32)
    new_estimate = estimate + own_piece
    left_piece = jnp.roll(compressed, 1, axis=0).astype(jnp.float32)
    right_piece = jnp.roll(compressed, -1, axis=0).astype(jnp.float32)
    weight_right = edge_weight
    weight_left = jnp.roll(edge_weight, 1)
    weight_self = 1.0 - weight_left - weight_right
    new_mixed = mixed_sum + weight_self[:, None, None] * own_piece
    new_mixed = new_mixed + weight_left[:, None, None] * left_piece
    new_mixed = new_mixed + weight_right[:, None, None] * right_piece
    new_params = stepped + mixing_rate * (new_mixed - new_estimate)
    return (new_params, new_estimate, new_mixed)
```

```python
import functools
import math

import jax
import jax.numpy as jnp
from jax import lax
from jax.experimental import pallas as pl
from jax.experimental.pallas import tpu as pltpu
from jax.sharding import PartitionSpec as P

step_size = 0.5
mixing_rate = 0.4
CHUNKS = 8
MESH = pl.DeviceIdType.MESH
f32 = jnp.float32
bf16 = jnp.bfloat16


def kernel(
    cfg,
    params, estimate, mixed, acts, grads, exponents, edges,
    out_params, out_estimate, out_mixed,
    act_v, act_t, grad_v, par_v, est_v, mix_v, new_p, new_e, new_m,
    mine, give, got, ring_out, ring_in, own, near, far,
    act_sem, grad_sem, par_sem, est_sem, mix_sem, put_sem,
    pair_s, pair_r, ring_s, ring_r, near_s, near_r, far_s, far_r,
):
    members, groups, chunks, rows, width, tokens, factor = cfg
    chips = members // 2
    hops = chips // 2
    cols = width // chunks
    half = rows // 2
    g = lax.axis_index("grp")
    m = lax.axis_index("mem")
    chip, core = m // 2, m % 2
    other = 1 - core
    sibling = chip * 2 + other
    ring_to = [
        lax.rem(chip + 1, chips) * 2 + core,
        lax.rem(chip + chips - 1, chips) * 2 + core,
    ]
    odd = g % 2
    partner = g + 1 - 2 * odd
    onward = lax.rem(g + 2 - 4 * odd + groups, groups)
    backward = lax.rem(g + groups - 2 + 4 * odd, groups)

    def act_copy(block):
        return pltpu.make_async_copy(
            acts.at[:, pl.ds(pl.multiple_of(block * rows, rows), rows)],
            act_v.at[block],
            act_sem.at[block],
        )

    def chunk_of(ref, j):
        return ref.at[:, pl.ds(pl.multiple_of(j * cols, cols), cols)]

    def grad_copy(j):
        return pltpu.make_async_copy(chunk_of(grads, j), grad_v.at[j], grad_sem.at[j])

    def load_copies(j):
        return [
            pltpu.make_async_copy(chunk_of(src.at[0], j), dst.at[j], sem.at[j])
            for src, dst, sem in (
                (params, par_v, par_sem), (estimate, est_v, est_sem), (mixed, mix_v, mix_sem)
            )
        ]

    def put_copy(which, j):
        src, dst = ((new_p, out_params), (new_e, out_estimate), (new_m, out_mixed))[which]
        return pltpu.make_async_copy(src.at[j], chunk_of(dst.at[0], j), put_sem.at[which, j])

    def pair_copy(j):
        return pltpu.make_async_remote_copy(
            src_ref=give.at[j], dst_ref=got.at[j],
            send_sem=pair_s.at[j], recv_sem=pair_r.at[j],
            device_id={"mem": sibling}, device_id_type=MESH,
        )

    def ring_copy(s, way, j):
        part = pl.ds(way * half, half) if s == 0 else pl.ds(0, rows)
        return pltpu.make_async_remote_copy(
            src_ref=ring_out.at[s, way, j, part],
            dst_ref=ring_in.at[s, way, j, part],
            send_sem=ring_s.at[s, way, j], recv_sem=ring_r.at[s, way, j],
            device_id={"mem": ring_to[way]}, device_id_type=MESH,
        )

    def near_copy(j):
        return pltpu.make_async_remote_copy(
            src_ref=own.at[j], dst_ref=near.at[j],
            send_sem=near_s.at[j], recv_sem=near_r.at[j],
            device_id={"grp": partner}, device_id_type=MESH,
        )

    def far_copy(j):
        return pltpu.make_async_remote_copy(
            src_ref=near.at[j], dst_ref=far.at[j],
            send_sem=far_s.at[j], recv_sem=far_r.at[j],
            device_id={"grp": onward}, device_id_type=MESH,
        )

    def blocks_of(parity):
        return lambda c: c * 2 + parity

    for c in range(chips):
        act_copy(c * 2 + other).start()
    grad_copy(0).start()
    for c in range(chips):
        act_copy(c * 2 + core).start()
    for j in range(1, chunks):
        grad_copy(j).start()
    for j in range(chunks):
        for copy in load_copies(j):
            copy.start()

    barrier = pltpu.get_barrier_semaphore()
    for peer in (
        {"mem": sibling}, {"mem": ring_to[0]}, {"mem": ring_to[1]},
        {"grp": partner}, {"grp": onward}, {"grp": backward},
    ):
        pl.semaphore_signal(barrier, inc=1, device_id=peer, device_id_type=MESH)
    pl.semaphore_wait(barrier, 6)

    def turn(parity):
        def body(c, carry):
            act_copy(c * 2 + parity).wait()
            start = pl.multiple_of(c * rows, rows)
            act_t[parity, pl.ds(start, rows), :] = act_v[c * 2 + parity].T
            return carry

        lax.fori_loop(0, chips, body, 0)

    def multiply(parity, j, into):
        into[j] = jnp.dot(act_t[parity], grad_v[j], preferred_element_type=f32).astype(bf16)

    def stage_multiply(j):
        @pl.when(j == 0)
        def _():
            turn(other)

        grad_copy(j).wait()
        multiply(other, j, give)
        pair_copy(j).start()

        @pl.when(j == 0)
        def _():
            turn(core)

        multiply(core, j, mine)

    def pair_sum(j, dest, start, count):
        at = pl.ds(pl.multiple_of(dest * rows + start, half), count)
        return mine[j, at, :].astype(f32) + got[j, at, :].astype(f32)

    def dest_of(s, way):
        ahead = hops - s
        return lax.rem(chip + (ahead if way == 0 else chips - ahead), chips)

    def stage_first(j):
        pair_copy(j).wait_recv()
        for way in (0, 1):
            ring_out[0, way, j, pl.ds(way * half, half), :] = pair_sum(
                j, dest_of(0, way), way * half, half
            ).astype(bf16)
            ring_copy(0, way, j).start()

    def stage_ring(s, j):
        for way in (0, 1):
            ring_copy(s - 1, way, j).wait_recv()
            for part in (0, 1):
                total = pair_sum(j, dest_of(s, way), part * half, half)
                if s >= 2 or part == way:
                    total = total + ring_in[s - 1, way, j, pl.ds(part * half, half), :].astype(f32)
                ring_out[s, way, j, pl.ds(part * half, half), :] = total.astype(bf16)
            ring_copy(s, way, j).start()

    weight_right = edges[g]
    weight_left = edges[lax.rem(g + groups - 1, groups)]
    weight_self = 1.0 - weight_left - weight_right
    weight_near = jnp.where(odd == 1, weight_left, weight_right)
    weight_far = jnp.where(odd == 1, weight_right, weight_left)
    blocks = exponents.shape[1]
    block_rows = rows // blocks

    def stage_compress(j):
        for way in (0, 1):
            ring_copy(hops - 1, way, j).wait_recv()
        for copy in load_copies(j):
            copy.wait()
        for b in range(blocks):
            exponent = exponents[0, b]
            scale = (jnp.int32(1) << exponent).astype(f32)
            inverse = (jnp.int32(1) << (15 - exponent)).astype(f32) * (2.0 ** -15)
            at = pl.ds(b * block_rows, block_rows)
            here = pl.ds(pl.multiple_of(chip * rows + b * block_rows, block_rows), block_rows)
            gradient = (
                mine[j, here, :].astype(f32)
                + got[j, here, :].astype(f32)
                + ring_in[hops - 1, 0, j, at, :].astype(f32)
                + ring_in[hops - 1, 1, j, at, :].astype(f32)
            )
            stepped = par_v[j, at, :] - factor * gradient
            base = est_v[j, at, :]
            levels = jnp.clip((stepped - base) * inverse, -1.0, 1.0).astype(bf16)
            compressed = levels.astype(f32) * scale
            own[j, at, :] = compressed.astype(bf16)
            new_p[j, at, :] = stepped
            new_e[j, at, :] = base + compressed
            new_m[j, at, :] = mix_v[j, at, :] + weight_self * compressed
        near_copy(j).start()
        put_copy(1, j).start()

    def stage_forward(j):
        near_copy(j).wait_recv()
        far_copy(j).start()

    def stage_finish(j):
        far_copy(j).wait_recv()
        total = (
            new_m[j] + weight_near * near[j].astype(f32) + weight_far * far[j].astype(f32)
        )
        new_m[j] = total
        new_p[j] = new_p[j] + mixing_rate * (total - new_e[j])
        put_copy(2, j).start()
        put_copy(0, j).start()

    stages = [(stage_multiply, 0), (stage_first, 1)]
    for s in range(1, hops):
        stages.append((functools.partial(stage_ring, s), 1 + s))
    stages += [(stage_compress, 1 + hops), (stage_forward, 2 + hops), (stage_finish, 3 + hops)]
    order = stages[1:] + stages[:1]

    def body(t, carry):
        for stage, lag in order:
            j = t - lag

            @pl.when(jnp.logical_and(j >= 0, j < chunks))
            def _(stage=stage, j=j):
                stage(j)

        return carry

    lax.fori_loop(0, chunks + 3 + hops, body, 0)

    def drain(j, carry):
        pair_copy(j).wait_send()
        for s in range(hops):
            for way in (0, 1):
                ring_copy(s, way, j).wait_send()
        near_copy(j).wait_send()
        far_copy(j).wait_send()
        for which in range(3):
            put_copy(which, j).wait()
        return carry

    lax.fori_loop(0, chunks, drain, 0)


def on_device(members, groups, params, estimate, mixed, acts, grads, exponents, edges):
    rows, width = params.shape[1:]
    tokens = acts.shape[0]
    chunks = CHUNKS
    cols = width // chunks
    chips = members // 2
    hops = chips // 2
    factor = step_size / math.sqrt(members * tokens)
    cfg = (members, groups, chunks, rows, width, tokens, factor)
    wide = (chunks, rows, cols)
    tall = (chunks, chips * rows, cols)
    dma = pltpu.SemaphoreType.DMA
    any_spec = pl.BlockSpec(memory_space=pl.ANY)
    smem = pl.BlockSpec(memory_space=pltpu.SMEM)
    return pl.pallas_call(
        functools.partial(kernel, cfg),
        out_shape=[jax.ShapeDtypeStruct(params.shape, f32)] * 3,
        in_specs=[any_spec] * 5 + [smem] * 2,
        out_specs=[any_spec] * 3,
        scratch_shapes=[
            pltpu.VMEM((members, tokens, rows), bf16),
            pltpu.VMEM((2, chips * rows, tokens), bf16),
            pltpu.VMEM((chunks, tokens, cols), bf16),
            *[pltpu.VMEM(wide, f32)] * 6,
            *[pltpu.VMEM(tall, bf16)] * 3,
            *[pltpu.VMEM((hops, 2) + wide, bf16)] * 2,
            *[pltpu.VMEM(wide, bf16)] * 3,
            dma((members,)), dma((chunks,)), dma((chunks,)), dma((chunks,)), dma((chunks,)),
            dma((3, chunks)),
            dma((chunks,)), dma((chunks,)),
            dma((hops, 2, chunks)), dma((hops, 2, chunks)),
            dma((chunks,)), dma((chunks,)), dma((chunks,)), dma((chunks,)),
        ],
        compiler_params=pltpu.CompilerParams(
            collective_id=0, has_side_effects=True, vmem_limit_bytes=66 * 1000 * 1000
        ),
    )(params, estimate, mixed, acts, grads, exponents, edges)


def solution(mesh):
    shard = P("grp", "mem", None)
    tokens = P(("grp", "mem"), None)
    return jax.shard_map(
        functools.partial(on_device, mesh.shape["mem"], mesh.shape["grp"]),
        mesh=mesh,
        in_specs=(shard, shard, shard, tokens, tokens, P("grp", "mem"), P()),
        out_specs=(shard, shard, shard),
        check_vma=False,
    )
```

```python
import functools
import math

import jax
import jax.numpy as jnp
from jax import lax
from jax.experimental import pallas as pl
from jax.experimental.pallas import tpu as pltpu
from jax.sharding import PartitionSpec as P

step_size = 0.5
mixing_rate = 0.4
CHUNKS = 8
DEPTH = 3
LAG = 2
MESH = pl.DeviceIdType.MESH
f32 = jnp.float32
bf16 = jnp.bfloat16


def kernel(
    cfg,
    params, estimate, mixed, acts, grads, exponents, edges,
    out_params, out_estimate, out_mixed,
    act_v, act_t, grad_v, par_v, est_v, mix_v,
    mine, give, got, line_out, line_in, own, near, far,
    act_sem, grad_sem, par_sem, est_sem, mix_sem,
    pair_s, pair_r, line_s, line_r, near_s, near_r, far_s, far_r,
):
    members, groups, chunks, rows, width, tokens, factor = cfg
    chips = members // 2
    pairs = chips // 2
    items = pairs * chunks
    slots = (chips - 1) * chunks
    cols = width // chunks
    g = lax.axis_index("grp")
    m = lax.axis_index("mem")
    chip, core = m // 2, m % 2
    other = 1 - core
    sibling = chip * 2 + other
    line_to = [
        lax.rem(chip + 1, chips) * 2 + core,
        lax.rem(chip + chips - 1, chips) * 2 + core,
    ]
    place = [chip, chips - 1 - chip]
    odd = g % 2
    partner = g + 1 - 2 * odd
    onward = lax.rem(g + 2 - 4 * odd + groups, groups)
    backward = lax.rem(g + groups - 2 + 4 * odd, groups)

    def act_copy(block):
        return pltpu.make_async_copy(
            acts.at[:, pl.ds(pl.multiple_of(block * rows, rows), rows)],
            act_v.at[block],
            act_sem.at[block],
        )

    def chunk_of(ref, j):
        return ref.at[:, pl.ds(pl.multiple_of(j * cols, cols), cols)]

    def grad_copy(j):
        return pltpu.make_async_copy(chunk_of(grads, j), grad_v.at[j], grad_sem.at[j])

    def load_copies(j):
        return [
            pltpu.make_async_copy(chunk_of(src.at[0], j), dst.at[j], sem.at[j])
            for src, dst, sem in (
                (params, par_v, par_sem), (estimate, est_v, est_sem), (mixed, mix_v, mix_sem)
            )
        ]

    def lanes(j):
        return pl.ds(pl.multiple_of(j * cols, cols), cols)

    def pair_copy(i):
        return pltpu.make_async_remote_copy(
            src_ref=give.at[i], dst_ref=got.at[i],
            send_sem=pair_s.at[i], recv_sem=pair_r.at[i],
            device_id={"mem": sibling}, device_id_type=MESH,
        )

    def line_copy(way, slot):
        return pltpu.make_async_remote_copy(
            src_ref=line_out.at[way, slot], dst_ref=line_in.at[way, slot],
            send_sem=line_s.at[way, slot], recv_sem=line_r.at[way, slot],
            device_id={"mem": line_to[way]}, device_id_type=MESH,
        )

    def near_copy(j):
        return pltpu.make_async_remote_copy(
            src_ref=own.at[j], dst_ref=near.at[j],
            send_sem=near_s.at[j], recv_sem=near_r.at[j],
            device_id={"grp": partner}, device_id_type=MESH,
        )

    def far_copy(j):
        return pltpu.make_async_remote_copy(
            src_ref=near.at[j], dst_ref=far.at[j],
            send_sem=far_s.at[j], recv_sem=far_r.at[j],
            device_id={"grp": onward}, device_id_type=MESH,
        )

    def members_of(b):
        return [(b, other), (chips - 1 - b, other), (b, core), (chips - 1 - b, core)]

    barrier = pltpu.get_barrier_semaphore()
    for peer in (
        {"mem": sibling}, {"mem": line_to[0]}, {"mem": line_to[1]},
        {"grp": partner}, {"grp": onward}, {"grp": backward},
    ):
        pl.semaphore_signal(barrier, inc=1, device_id=peer, device_id_type=MESH)

    grad_copy(0).start()
    for b in range(pairs):
        for dest, parity in members_of(b):
            act_copy(dest * 2 + parity).start()
        if b == 0:
            for j in range(1, chunks):
                grad_copy(j).start()
    for j in range(chunks):
        for copy in load_copies(j):
            copy.start()

    def multiply(i, before_send):
        b, j = i // chunks, i % chunks

        @pl.when(b == 0)
        def _():
            grad_copy(j).wait()

        def turn(dest, parity):
            @pl.when(j == 0)
            def _():
                block = dest * 2 + parity
                act_copy(block).wait()
                act_t[block] = act_v[block].T

        def product(dest, parity):
            return jnp.dot(
                act_t[dest * 2 + parity], grad_v[j], preferred_element_type=f32
            ).astype(bf16)

        for which, dest in ((0, b), (1, chips - 1 - b)):
            turn(dest, other)
            give[i, which] = product(dest, other)
        before_send()
        pair_copy(i).start()
        for which, dest in ((0, b), (1, chips - 1 - b)):
            turn(dest, core)
            mine[i, which] = product(dest, core)

    def pair_sum(i, which):
        return mine[i, which].astype(f32) + got[i, which].astype(f32)

    def pass_on(way, t):
        slot = t - LAG * place[way]
        block = slot // chunks
        j = slot % chunks

        @pl.when(jnp.logical_and(slot >= 0, slot < (chips - 1 - place[way]) * chunks))
        def _():
            @pl.when(slot >= DEPTH)
            def _():
                line_copy(way, slot - DEPTH).wait_send()

            late = block >= pairs
            i = jnp.where(late, chips - 1 - block, block) * chunks + j
            which = jnp.where(late, way, 1 - way)

            @pl.when(place[way] == 0)
            def _():
                line_out[way, slot] = pair_sum(i, which).astype(bf16)

            @pl.when(place[way] > 0)
            def _():
                line_copy(way, slot).wait_recv()
                line_out[way, slot] = (
                    pair_sum(i, which) + line_in[way, slot].astype(f32)
                ).astype(bf16)

            line_copy(way, slot).start()

    weight_right = edges[g]
    weight_left = edges[lax.rem(g + groups - 1, groups)]
    weight_self = 1.0 - weight_left - weight_right
    weight_near = jnp.where(odd == 1, weight_left, weight_right)
    weight_far = jnp.where(odd == 1, weight_right, weight_left)
    blocks = exponents.shape[1]
    block_rows = rows // blocks
    first = jnp.int32(0)
    for c in range(chips):
        after = [(chips - 1 - c) * chunks + LAG * c] if c > 0 else []
        if c < chips - 1:
            after.append(c * chunks + LAG * (chips - 1 - c))
        first = jnp.where(chip == c, max(after), first)
    own_which = jnp.where(chip >= pairs, 1, 0)
    own_block = jnp.where(chip >= pairs, chips - 1 - chip, chip)

    def compress(j):
        slot_of = [(chips - 1 - place[way]) * chunks + j for way in (0, 1)]
        for way in (0, 1):
            @pl.when(place[way] > 0)
            def _(way=way):
                line_copy(way, slot_of[way]).wait_recv()

            @pl.when(place[way] == 0)
            def _(way=way):
                line_in[way, slot_of[way]] = jnp.zeros((rows, cols), bf16)

        for copy in load_copies(j):
            copy.wait()
        i = own_block * chunks + j
        for b in range(blocks):
            exponent = exponents[0, b]
            scale = (jnp.int32(1) << exponent).astype(f32)
            inverse = (jnp.int32(1) << (15 - exponent)).astype(f32) * (2.0 ** -15)
            at = pl.ds(b * block_rows, block_rows)
            gradient = (
                mine[i, own_which, at, :].astype(f32)
                + got[i, own_which, at, :].astype(f32)
                + line_in[0, slot_of[0], at, :].astype(f32)
                + line_in[1, slot_of[1], at, :].astype(f32)
            )
            stepped = par_v[j, at, :] - factor * gradient
            base = est_v[j, at, :]
            levels = jnp.clip((stepped - base) * inverse, -1.0, 1.0).astype(bf16)
            compressed = levels.astype(f32) * scale
            own[j, at, :] = compressed.astype(bf16)
            out_params[0, at, lanes(j)] = stepped
            out_estimate[0, at, lanes(j)] = base + compressed
            out_mixed[0, at, lanes(j)] = mix_v[j, at, :] + weight_self * compressed
        near_copy(j).start()

    def forward(j):
        near_copy(j).wait_recv()
        far_copy(j).start()

    def finish(j):
        far_copy(j).wait_recv()
        total = (
            out_mixed[0, :, lanes(j)] + weight_near * near[j].astype(f32) + weight_far * far[j].astype(f32)
        )
        out_mixed[0, :, lanes(j)] = total
        out_params[0, :, lanes(j)] = out_params[0, :, lanes(j)] + mixing_rate * (
            total - out_estimate[0, :, lanes(j)]
        )

    def guarded(run, j, count):
        @pl.when(jnp.logical_and(j >= 0, j < count))
        def _():
            run(j)

    multiply(0, lambda: pl.semaphore_wait(barrier, 6))
    multiply(1, lambda: None)

    def body(t, carry):
        guarded(lambda i: pair_copy(i).wait_recv(), t, items)
        for way in (0, 1):
            pass_on(way, t)
        guarded(compress, t - first, chunks)
        guarded(forward, t - first - LAG, chunks)
        guarded(finish, t - first - 2 * LAG, chunks)
        guarded(lambda i: multiply(i, lambda: None), t + 2, items)
        return carry

    lax.fori_loop(0, slots + LAG * (chips + 1), body, 0)

    def drain_pair(i, carry):
        pair_copy(i).wait_send()
        return carry

    def drain_line(slot, carry):
        for way in (0, 1):
            count = (chips - 1 - place[way]) * chunks

            @pl.when(jnp.logical_and(slot < count, slot >= count - DEPTH))
            def _(way=way):
                line_copy(way, slot).wait_send()
        return carry

    def drain(j, carry):
        near_copy(j).wait_send()
        far_copy(j).wait_send()
        return carry

    lax.fori_loop(0, items, drain_pair, 0)
    lax.fori_loop(0, slots, drain_line, 0)
    lax.fori_loop(0, chunks, drain, 0)


def on_device(members, groups, params, estimate, mixed, acts, grads, exponents, edges):
    rows, width = params.shape[1:]
    tokens = acts.shape[0]
    chunks = CHUNKS
    cols = width // chunks
    chips = members // 2
    items = chips // 2 * chunks
    slots = (chips - 1) * chunks
    factor = step_size / math.sqrt(members * tokens)
    cfg = (members, groups, chunks, rows, width, tokens, factor)
    wide = (chunks, rows, cols)
    tall = (items, 2, rows, cols)
    dma = pltpu.SemaphoreType.DMA
    any_spec = pl.BlockSpec(memory_space=pl.ANY)
    smem = pl.BlockSpec(memory_space=pltpu.SMEM)
    return pl.pallas_call(
        functools.partial(kernel, cfg),
        out_shape=[pltpu.VMEM(params.shape, f32)] * 3,
        in_specs=[any_spec] * 5 + [smem] * 2,
        out_specs=[pl.BlockSpec(memory_space=pltpu.VMEM)] * 3,
        scratch_shapes=[
            pltpu.VMEM((members, tokens, rows), bf16),
            pltpu.VMEM((members, rows, tokens), bf16),
            pltpu.VMEM((chunks, tokens, cols), bf16),
            *[pltpu.VMEM(wide, f32)] * 3,
            *[pltpu.VMEM(tall, bf16)] * 3,
            pltpu.VMEM((2, slots, rows, cols), bf16),
            pltpu.VMEM((2, slots + chunks, rows, cols), bf16),
            *[pltpu.VMEM(wide, bf16)] * 3,
            dma((members,)), dma((chunks,)), dma((chunks,)), dma((chunks,)), dma((chunks,)),
            dma((items,)), dma((items,)), dma((2, slots)), dma((2, slots)),
            dma((chunks,)), dma((chunks,)), dma((chunks,)), dma((chunks,)),
        ],
        compiler_params=pltpu.CompilerParams(
            collective_id=0, has_side_effects=True, vmem_limit_bytes=53 * 1024 * 1024
        ),
    )(params, estimate, mixed, acts, grads, exponents, edges)


def solution(mesh):
    shard = P("grp", "mem", None)
    tokens = P(("grp", "mem"), None)
    return jax.shard_map(
        functools.partial(on_device, mesh.shape["mem"], mesh.shape["grp"]),
        mesh=mesh,
        in_specs=(shard, shard, shard, tokens, tokens, P("grp", "mem"), P()),
        out_specs=(shard, shard, shard),
        check_vma=False,
    )
```
